32 devices in a mesh: dp: 2 (over z, core), ep: 16 (over x, y).
Axes of the slice: x: 4, y: 4, z: 1, core: 2. Of those that a mesh axis runs over, the one named last changes fastest.
The devices are a block of a 4x4x8 slice.
Arguments:
- x: bfloat16 [2, 16, 256, 2048], P('dp', 'ep'), parts along dimension 0
- expert: int32 [2, 16, 256, 6], P('dp', 'ep'), parts along dimension 0
- slot: int32 [2, 16, 256, 6], P('dp', 'ep'), parts along dimension 0
- gate: float32 [2, 16, 256, 6], P('dp', 'ep'), parts along dimension 0
- w_gate: bfloat16 [64, 2048, 1408], P('ep')
- w_up: bfloat16 [64, 2048, 1408], P('ep')
- w_down: bfloat16 [64, 1408, 2048], P('ep')
- s_gate: bfloat16 [2048, 2816], replicated
- s_up: bfloat16 [2048, 2816], replicated
- s_down: bfloat16 [2816, 2048], replicated
Outputs:
- y: bfloat16 [2, 16, 256, 2048], P('dp', 'ep'), parts along dimension 0
There are 2 independent parts. The reference program is written for one: setup_inputs(seed, part) draws one part's arguments, and reference() takes and returns one part's arrays. A program takes and returns all parts, laid end to end along the dimension named above; an argument that names none is the same for every part.
All inputs are finite; a program needn't handle non-finite values.
Results may differ from the reference program's by a relative error of at most 0.009.
Values are sent between devices in bfloat16 or wider.
A program may use at most 768 MiB of HBM per device.

```python
import jax
import jax.numpy as jnp

MEMBERS = 16
TOKENS = 256
D = 2048
FF = 1408
TOP = 6
EXPERTS = 64
SHARED_FF = 2816
SLOTS = 5 * TOKENS * TOP // (4 * EXPERTS)


def setup_inputs(seed: int = 0, part: int = 0) -> dict:
    own, k1, k2, k3, k4, k5, k6 = jax.random.split(jax.random.key(seed), 7)
    kx, ke, kl, kg = jax.random.split(jax.random.fold_in(own, part), 4)
    devices = (1, MEMBERS)
    place = jax.random.permutation(kl, jnp.arange(EXPERTS, dtype=jnp.uint32))
    slow = ((EXPERTS + (9 * place) % EXPERTS) << ((9 * place) // EXPERTS)) // EXPERTS
    wait = (jax.random.bits(ke, (*devices, TOKENS, EXPERTS), jnp.uint32) >> 10) * slow
    expert = jnp.argsort(wait, axis=-1)[..., :TOP].astype(jnp.int32)
    chosen = jax.nn.one_hot(expert, EXPERTS, dtype=jnp.int32)
    in_line = jnp.cumsum(chosen.reshape(*devices, TOKENS * TOP, EXPERTS), axis=2) - 1
    slot = jnp.sum(in_line.reshape(chosen.shape) * chosen, axis=-1)

    def one(key, rows, columns):
        return (jax.random.normal(key, (rows, columns), jnp.float32) * rows**-0.5).astype(jnp.bfloat16)

    def weights(key, rows, columns):
        return jax.lax.map(lambda k: one(k, rows, columns), jax.random.split(key, EXPERTS))

    return {
        "x": jax.random.normal(kx, (*devices, TOKENS, D), jnp.float32).astype(jnp.bfloat16),
        "expert": expert,
        "slot": slot,
        "gate": jax.nn.softmax(jax.random.normal(kg, expert.shape, jnp.float32)),
        "w_gate": weights(k1, D, FF),
        "w_up": weights(k2, D, FF),
        "w_down": weights(k3, FF, D),
        "s_gate": one(k4, D, SHARED_FF),
        "s_up": one(k5, D, SHARED_FF),
        "s_down": one(k6, SHARED_FF, D),
    }


def einsum(form, a, b):
    return jnp.einsum(form, a.astype(jnp.float32), b.astype(jnp.float32))


def for_all(x, s_gate, s_up, s_down):
    h = jax.nn.silu(einsum("...d,df->...f", x, s_gate)) * einsum("...d,df->...f", x, s_up)
    return einsum("...f,fd->...d", h.astype(jnp.bfloat16), s_down)


def reference(x, expert, slot, gate, w_gate, w_up, w_down, s_gate, s_up, s_down):
    to_expert = jax.nn.one_hot(expert, EXPERTS, dtype=jnp.bfloat16)
    to_slot = jax.nn.one_hot(slot, SLOTS, dtype=jnp.bfloat16)
    weighted = to_expert * gate[..., None].astype(jnp.bfloat16)
    dispatch = einsum("abtke,abtkc->abtec", to_expert, to_slot).astype(jnp.bfloat16)
    combine = einsum("abtke,abtkc->abtec", weighted, to_slot).astype(jnp.bfloat16)
    z = einsum("abtec,abtd->aebcd", dispatch, x).astype(jnp.bfloat16)
    h = jax.nn.silu(einsum("aebcd,edf->aebcf", z, w_gate))
    h = (h * einsum("aebcd,edf->aebcf", z, w_up)).astype(jnp.bfloat16)
    out = einsum("aebcf,efd->aebcd", h, w_down).astype(jnp.bfloat16)
    y = einsum("abtec,aebcd->abtd", combine, out)
    return (y + for_all(x, s_gate, s_up, s_down)).astype(jnp.bfloat16)
```

```python
import functools
import math

import jax
import jax.numpy as jnp
from jax import lax
from jax.experimental import pallas as pl
from jax.experimental.pallas import tpu as pltpu
from jax.sharding import PartitionSpec as P

MESH = pl.DeviceIdType.MESH
F32, BF16 = jnp.float32, jnp.bfloat16


def dot(a, b):
    return jnp.dot(a, b, preferred_element_type=F32)


def gated(g, u):
    return (jax.nn.silu(g) * u).astype(BF16)


class Place:
    def __init__(self, side):
        me = lax.axis_index("ep")
        self.side = side
        self.x, self.y = lax.div(me, side), lax.rem(me, side)

    def peer(self, axis, d):
        if axis == 0:
            c = lax.rem(self.x + d, self.side)
            return c, {"ep": c * self.side + self.y}
        c = lax.rem(self.y + d, self.side)
        return c, {"ep": self.x * self.side + c}

    def greet(self):
        barrier = pltpu.get_barrier_semaphore()
        for axis in (0, 1):
            for d in range(1, self.side):
                pl.semaphore_signal(barrier, inc=1, device_id=self.peer(axis, d)[1], device_id_type=MESH)
        pl.semaphore_wait(barrier, 2 * (self.side - 1))


def remote(src, dst, sems, k, device):
    return pltpu.make_async_remote_copy(
        src_ref=src, dst_ref=dst, send_sem=sems[0].at[k], recv_sem=sems[1].at[k], device_id=device, device_id_type=MESH
    )


def dispatch_kernel(side, x_ref, ra_ref, rb_ref, sg_ref, su_ref, sd_ref, z_ref, ga_ref, gb_ref, sh_ref,
                    gxa, gxb, sta, stb, s1s, s1r, s2s, s2r, loc):
    at = Place(side)
    tokens, half = gxa.shape[1:]
    local = z_ref.shape[0]
    pad = z_ref.shape[3]
    at.greet()

    first = []
    for axis, (lo, gx, r, g) in enumerate(((0, gxa, ra_ref, ga_ref), (half, gxb, rb_ref, gb_ref))):
        mine = (at.x, at.y)[axis]
        for d in range(1, side):
            c, device = at.peer(axis, d)
            k = (axis * side + d) * 2
            first.append(remote(r.at[c], g.at[mine], (s1s, s1r), k, device))
            first.append(remote(x_ref.at[:, pl.ds(lo, half)], gx.at[mine], (s1s, s1r), k + 1, device))
    for c in first:
        c.start()
    gxa[at.x] = x_ref[:, :half]
    gxb[at.y] = x_ref[:, half:]
    ga_ref[at.x] = ra_ref[at.x]
    gb_ref[at.y] = rb_ref[at.y]

    sh_ref[...] = jnp.zeros_like(sh_ref)

    def shared(g_ref, u_ref, d_ref):
        x = x_ref[...]
        sh_ref[...] += dot(gated(dot(x, g_ref[...]), dot(x, u_ref[...])), d_ref[...])

    d_model, ff = sg_ref.shape
    tile = 256 if ff % 256 == 0 else 128
    pltpu.emit_pipeline(
        shared,
        grid=(ff // tile,),
        in_specs=[
            pl.BlockSpec((d_model, tile), lambda i: (0, i)),
            pl.BlockSpec((d_model, tile), lambda i: (0, i)),
            pl.BlockSpec((tile, d_model), lambda i: (i, 0)),
        ],
    )(sg_ref, su_ref, sd_ref)

    for c in first:
        c.wait()

    def second(e):
        out, own = [], []
        for axis, st in enumerate((sta, stb)):
            for d in range(side):
                c, device = at.peer(1 - axis, d)
                if axis == 0:
                    dst = z_ref.at[e, at.y, :, :, pl.ds(0, half)]
                else:
                    dst = z_ref.at[e, :, at.x, :, pl.ds(half, half)]
                if d == 0:
                    own.append(pltpu.make_async_copy(st.at[e, c], dst, loc.at[e, axis]))
                else:
                    out.append(remote(st.at[e, c], dst, (s2s, s2r), (e * 2 + axis) * side + d, device))
        return out, own

    token = lax.broadcasted_iota(jnp.int32, (tokens, side * pad), 0).astype(F32) + 1.0

    @pl.loop(0, local)
    def _(e):
        for gx, g, st in ((gxa, ga_ref, sta), (gxb, gb_ref, stb)):
            for s in range(side):
                pick = (token == g[s, pl.ds(e, 1), :]).astype(BF16)
                rows = lax.dot_general(pick, gx[s], (((0,), (0,)), ((), ())), preferred_element_type=F32)
                rows = rows.astype(BF16)
                for c in range(side):
                    st[e, c, s] = rows[c * pad : (c + 1) * pad]
        out, own = second(e)
        for c in out + own:
            c.start()

    @pl.loop(0, local)
    def _(e):
        out, own = second(e)
        for c in out + own:
            c.wait()


def expert_kernel(z_ref, wg_ref, wu_ref, wd_ref, out_ref, h_ref):
    z = z_ref[0]
    ff, d_model = wd_ref.shape[1:]
    for lo in range(0, ff, 512):
        hi = min(lo + 512, ff)
        h_ref[:, lo:hi] = gated(dot(z, wg_ref[0, :, lo:hi]), dot(z, wu_ref[0, :, lo:hi]))
    for lo in range(0, d_model, 512):
        hi = min(lo + 512, d_model)
        out_ref[0, :, lo:hi] = dot(h_ref[...], wd_ref[0, :, lo:hi]).astype(BF16)


def combine_kernel(side, o_ref, ga_ref, gb_ref, sh_ref, y_ref, ca, cb, pa, pb, qa, qb, ta, tb, s1s, s1r, s2s, s2r, loc):
    at = Place(side)
    local = ca.shape[0]
    pad, half = ca.shape[3:]
    tokens = pa.shape[1]
    at.greet()

    def first(e):
        out, own = [], []
        for axis in (0, 1):
            for d in range(side):
                c, device = at.peer(1 - axis, d)
                if axis == 0:
                    src, dst = o_ref.at[e, c, :, :, pl.ds(0, half)], ca.at[e, :, at.y]
                else:
                    src, dst = o_ref.at[e, :, c, :, pl.ds(half, half)], cb.at[e, :, at.x]
                if d == 0:
                    own.append(pltpu.make_async_copy(src, dst, loc.at[e, axis]))
                else:
                    out.append(remote(src, dst, (s1s, s1r), (e * 2 + axis) * side + d, device))
        return out + own

    @pl.loop(0, local)
    def _(e):
        for c in first(e):
            c.start()

    pa[...] = jnp.zeros_like(pa)
    pb[...] = jnp.zeros_like(pb)
    token = lax.broadcasted_iota(jnp.int32, (tokens, side * pad), 0).astype(F32) + 1.0

    @pl.loop(0, local)
    def _(e):
        for c in first(e):
            c.wait()
        for p, g, rows in ((pa, ga_ref, ca), (pb, gb_ref, cb)):
            for s in range(side):
                weigh = jnp.where(token == g[s, pl.ds(e, 1), :], g[s, pl.ds(local + e, 1), :], 0.0).astype(BF16)
                p[s] += dot(weigh, rows[e, s].reshape(side * pad, half))

    second = []
    for axis, (p, t, q) in enumerate(((pa, ta, qa), (pb, tb, qb))):
        t[...] = p[...].astype(BF16)
        mine = (at.x, at.y)[axis]
        for d in range(1, side):
            c, device = at.peer(axis, d)
            second.append(remote(t.at[c], q.at[mine], (s2s, s2r), axis * side + d, device))
    for c in second:
        c.start()
    for c in second:
        c.wait()
    for axis, (p, q, lo) in enumerate(((pa, qa, 0), (pb, qb, half))):
        mine = (at.x, at.y)[axis]
        y = p[mine]
        for d in range(1, side):
            y += q[at.peer(axis, d)[0]].astype(F32)
        y_ref[:, lo : lo + half] = (y + sh_ref[:, lo : lo + half]).astype(BF16)


def solution(mesh):
    side = math.isqrt(mesh.shape["ep"])
    vmem, hbm = pl.BlockSpec(memory_space=pltpu.VMEM), pl.BlockSpec(memory_space=pl.ANY)
    dma = lambda *n: pltpu.SemaphoreType.DMA(n)
    limit = 62 << 20

    def body(x, expert, slot, gate, w_gate, w_up, w_down, s_gate, s_up, s_down):
        x, expert, slot, gate = x[0, 0], expert[0, 0], slot[0, 0], gate[0, 0]
        tokens, top = expert.shape
        d_model = x.shape[1]
        local, _, ff = w_gate.shape
        experts = local * side * side
        slots = 5 * tokens * top // (4 * experts)
        pad = -(-slots // 16) * 16
        half = d_model // 2
        assert tokens <= 256

        to_expert = jax.nn.one_hot(expert.reshape(-1), experts, dtype=BF16)
        slot = slot.reshape(-1)
        to_slot = jax.nn.one_hot(jnp.where(slot < slots, slot, pad), pad, dtype=BF16)
        number = jnp.repeat(jnp.arange(1, tokens + 1), top).astype(BF16)[:, None]
        held = jnp.concatenate([to_slot * number, to_slot * gate.reshape(-1).astype(BF16)[:, None]], axis=1)
        held = lax.dot_general(to_expert, held, (((0,), (0,)), ((), ())), preferred_element_type=F32)
        held = held.reshape(side, side, local, 2, pad)
        ra = held.transpose(0, 3, 2, 1, 4).reshape(side, 2 * local, side * pad)
        rb = held.transpose(1, 3, 2, 0, 4).reshape(side, 2 * local, side * pad)

        shape = jax.ShapeDtypeStruct
        z, ga, gb, sh = pl.pallas_call(
            functools.partial(dispatch_kernel, side),
            out_shape=(
                shape((local, side, side, pad, d_model), BF16),
                shape(ra.shape, F32),
                shape(rb.shape, F32),
                shape((tokens, d_model), F32),
            ),
            in_specs=[vmem, vmem, vmem, hbm, hbm, hbm],
            out_specs=(hbm, vmem, vmem, vmem),
            scratch_shapes=[
                pltpu.VMEM((side, tokens, half), BF16),
                pltpu.VMEM((side, tokens, half), BF16),
                pltpu.VMEM((local, side, side, pad, half), BF16),
                pltpu.VMEM((local, side, side, pad, half), BF16),
                dma(4 * side),
                dma(4 * side),
                dma(2 * local * side),
                dma(2 * local * side),
                dma(local, 2),
            ],
            compiler_params=pltpu.CompilerParams(collective_id=0, has_side_effects=True, vmem_limit_bytes=limit),
        )(x, ra, rb, s_gate, s_up, s_down)

        rows = side * side * pad
        out = pl.pallas_call(
            expert_kernel,
            grid=(local,),
            out_shape=shape((local, rows, d_model), BF16),
            in_specs=[
                pl.BlockSpec((1, rows, d_model), lambda e: (e, 0, 0)),
                pl.BlockSpec((1, d_model, ff), lambda e: (e, 0, 0)),
                pl.BlockSpec((1, d_model, ff), lambda e: (e, 0, 0)),
                pl.BlockSpec((1, ff, d_model), lambda e: (e, 0, 0)),
            ],
            out_specs=pl.BlockSpec((1, rows, d_model), lambda e: (e, 0, 0)),
            scratch_shapes=[pltpu.VMEM((rows, ff), BF16)],
            compiler_params=pltpu.CompilerParams(vmem_limit_bytes=limit),
        )(z.reshape(local, rows, d_model), w_gate, w_up, w_down)

        y = pl.pallas_call(
            functools.partial(combine_kernel, side),
            out_shape=shape((tokens, d_model), BF16),
            in_specs=[hbm, vmem, vmem, vmem],
            out_specs=vmem,
            scratch_shapes=[
                pltpu.VMEM((local, side, side, pad, half), BF16),
                pltpu.VMEM((local, side, side, pad, half), BF16),
                pltpu.VMEM((side, tokens, half), F32),
                pltpu.VMEM((side, tokens, half), F32),
                pltpu.VMEM((side, tokens, half), BF16),
                pltpu.VMEM((side, tokens, half), BF16),
                pltpu.VMEM((side, tokens, half), BF16),
                pltpu.VMEM((side, tokens, half), BF16),
                dma(2 * local * side),
                dma(2 * local * side),
                dma(2 * side),
                dma(2 * side),
                dma(local, 2),
            ],
            compiler_params=pltpu.CompilerParams(collective_id=1, has_side_effects=True, vmem_limit_bytes=limit),
        )(out.reshape(z.shape), ga, gb, sh)
        return y[None, None]

    token = P("dp", "ep")
    return jax.shard_map(
        body,
        mesh=mesh,
        in_specs=(token,) * 4 + (P("ep"),) * 3 + (P(),) * 3,
        out_specs=token,
        check_vma=False,
    )
```

```python
import functools
import math

import jax
import jax.numpy as jnp
from jax import lax
from jax.experimental import pallas as pl
from jax.experimental.pallas import tpu as pltpu
from jax.sharding import PartitionSpec as P

MESH = pl.DeviceIdType.MESH
F32, BF16 = jnp.float32, jnp.bfloat16
UP, DOWN = 128, 512
DEPTH = 3


def dot(a, b, contract=((1,), (0,))):
    return lax.dot_general(a, b, (contract, ((), ())), preferred_element_type=F32)


def gated(g, u):
    return (jax.nn.silu(g) * u).astype(BF16)


class Place:
    def __init__(self, side):
        me = lax.axis_index("ep")
        self.side = side
        self.x, self.y = lax.div(me, side), lax.rem(me, side)

    def peer(self, axis, d):
        if axis == 0:
            c = lax.rem(self.x + d, self.side)
            return c, {"ep": c * self.side + self.y}
        c = lax.rem(self.y + d, self.side)
        return c, {"ep": self.x * self.side + c}

    def greet(self):
        barrier = pltpu.get_barrier_semaphore()
        for axis in (0, 1):
            for d in range(1, self.side):
                pl.semaphore_signal(barrier, inc=1, device_id=self.peer(axis, d)[1], device_id_type=MESH)
        pl.semaphore_wait(barrier, 2 * (self.side - 1))


def remote(src, dst, sems, k, device):
    return pltpu.make_async_remote_copy(
        src_ref=src, dst_ref=dst, send_sem=sems[0].at[k], recv_sem=sems[1].at[k], device_id=device, device_id_type=MESH
    )


def tables(side, local, pad, slots, expert, slot, gate, ra, rb):
    top, tokens = expert.shape
    token = lax.broadcasted_iota(jnp.int32, (1, tokens), 1).astype(F32) + 1.0
    lines = lax.broadcasted_iota(jnp.int32, (side * local, tokens), 0)
    places = lax.broadcasted_iota(jnp.int32, (side * pad, tokens), 0)
    sums = [0.0, 0.0]
    for k in range(top):
        ex, sl = expert[k : k + 1], slot[k : k + 1]
        weight = gate[k : k + 1].astype(BF16).astype(F32)
        e, device = lax.rem(ex, local), lax.div(ex, local)
        where = lax.div(device, side), lax.rem(device, side)
        for axis in (0, 1):
            line = (lines == where[axis] * local + e).astype(F32).astype(BF16)
            hit = places == jnp.where(sl < slots, where[1 - axis] * pad + sl, -1)
            held = jnp.concatenate([jnp.where(hit, token, 0.0), jnp.where(hit, weight, 0.0)]).astype(BF16)
            sums[axis] += dot(line, held, ((1,), (1,)))
    for held, r in zip(sums, (ra, rb)):
        for c in range(side):
            r[c, :local] = held[c * local : (c + 1) * local, : side * pad]
            r[c, local:] = held[c * local : (c + 1) * local, side * pad :]


def layer_kernel(side, slots, x_ref, ex_ref, sl_ref, gt_ref, sg_ref, su_ref, sd_ref, wg_ref, wu_ref, wd_ref, y_ref,
                 ra, rb, ga, gb, gxa, gxb, sta, stb, z, h, ca, cb, pa, pb, ta, tb, qa, qb, sh, wup, wdn,
                 s1s, s1r, s2s, s2r, s3s, s3r, s4s, s4r, loc2, loc3, sup, sdn):
    at = Place(side)
    tokens, half = gxa.shape[1:]
    local, pad = z.shape[0], z.shape[3]
    rows = side * side * pad
    d_model, ff = wg_ref.shape[1:]
    ups, downs = ff // UP, d_model // DOWN

    def up_tile(n):
        e, i = lax.div(n, ups), lax.rem(n, ups)
        k = lax.rem(n, DEPTH)
        cols = pl.ds(pl.multiple_of(i * UP, UP), UP)
        return [
            pltpu.make_async_copy(w.at[e, :, cols], wup.at[k, :, pl.ds(j * UP, UP)], sup.at[k, j])
            for j, w in enumerate((wg_ref, wu_ref))
        ]

    def down_tile(n):
        e, i = lax.div(n, downs), lax.rem(n, downs)
        k = lax.rem(n, 2)
        cols = pl.ds(pl.multiple_of(i * DOWN, DOWN), DOWN)
        return pltpu.make_async_copy(wd_ref.at[e, :, cols], wdn.at[k], sdn.at[k])

    at.greet()

    first, small = [], []
    for axis, (lo, gx, r, g) in enumerate(((0, gxa, ra, ga), (half, gxb, rb, gb))):
        mine = (at.x, at.y)[axis]
        for d in range(1, side):
            c, device = at.peer(axis, d)
            k = (axis * side + d) * 2
            small.append(remote(r.at[c], g.at[mine], (s1s, s1r), k, device))
            first.append(remote(x_ref.at[:, pl.ds(lo, half)], gx.at[mine], (s1s, s1r), k + 1, device))
    for c in first:
        c.start()
    tables(side, local, pad, slots, ex_ref, sl_ref, gt_ref, ra, rb)
    gxa[at.x] = x_ref[:, :half]
    gxb[at.y] = x_ref[:, half:]
    sh[...] = jnp.zeros_like(sh)
    for c in small:
        c.start()
    ga[at.x] = ra[at.x]
    gb[at.y] = rb[at.y]

    def shared(g_ref, u_ref, d_ref):
        x = x_ref[...]
        sh[...] += dot(gated(dot(x, g_ref[...]), dot(x, u_ref[...])), d_ref[...])

    tile = 256 if sg_ref.shape[1] % 256 == 0 else 128
    pltpu.emit_pipeline(
        shared,
        grid=(sg_ref.shape[1] // tile,),
        in_specs=[
            pl.BlockSpec((d_model, tile), lambda i: (0, i)),
            pl.BlockSpec((d_model, tile), lambda i: (0, i)),
            pl.BlockSpec((tile, d_model), lambda i: (i, 0)),
        ],
    )(sg_ref, su_ref, sd_ref)

    for n in range(DEPTH - 1):
        for c in up_tile(jnp.int32(n)):
            c.start()
    down_tile(jnp.int32(0)).start()
    for c in small + first:
        c.wait()

    def second(e):
        out, own = [], []
        for axis, st in enumerate((sta, stb)):
            for d in range(side):
                c, device = at.peer(1 - axis, d)
                if axis == 0:
                    dst = z.at[e, at.y, :, :, pl.ds(0, half)]
                else:
                    dst = z.at[e, :, at.x, :, pl.ds(half, half)]
                if d == 0:
                    own.append(pltpu.make_async_copy(st.at[e, c], dst, loc2.at[e, axis]))
                else:
                    out.append(remote(st.at[e, c], dst, (s2s, s2r), (e * 2 + axis) * side + d, device))
        return out + own

    token = lax.broadcasted_iota(jnp.int32, (tokens, side * pad), 0).astype(F32) + 1.0

    @pl.loop(0, local)
    def _(e):
        for gx, g, st in ((gxa, ga, sta), (gxb, gb, stb)):
            for s in range(side):
                pick = (token == g[s, pl.ds(e, 1), :]).astype(F32).astype(BF16)
                picked = dot(pick, gx[s], ((0,), (0,))).astype(BF16)
                for c in range(side):
                    st[e, c, s] = picked[c * pad : (c + 1) * pad]
        for c in second(e):
            c.start()

    def third(e):
        out, own = [], []
        for axis in (0, 1):
            for d in range(side):
                c, device = at.peer(1 - axis, d)
                if axis == 0:
                    src, dst = z.at[e, c, :, :, pl.ds(0, half)], ca.at[e, :, at.y]
                else:
                    src, dst = z.at[e, :, c, :, pl.ds(half, half)], cb.at[e, :, at.x]
                if d == 0:
                    own.append(pltpu.make_async_copy(src, dst, loc3.at[e, axis]))
                else:
                    out.append(remote(src, dst, (s3s, s3r), (e * 2 + axis) * side + d, device))
        return out + own

    @pl.loop(0, local)
    def _(e):
        for c in second(e):
            c.wait()

        @pl.loop(0, ups)
        def _(i):
            n = e * ups + i

            @pl.when(n + DEPTH - 1 < local * ups)
            def _():
                for c in up_tile(n + DEPTH - 1):
                    c.start()

            for c in up_tile(n):
                c.wait()
            gu = dot(z[e].reshape(rows, d_model), wup[lax.rem(n, DEPTH)])
            h[:, pl.ds(pl.multiple_of(i * UP, UP), UP)] = gated(gu[:, :UP], gu[:, UP:])

        @pl.loop(0, downs)
        def _(i):
            n = e * downs + i

            @pl.when(n + 1 < local * downs)
            def _():
                down_tile(n + 1).start()

            down_tile(n).wait()
            out = dot(h[...], wdn[lax.rem(n, 2)]).astype(BF16)
            z[e, :, :, :, pl.ds(pl.multiple_of(i * DOWN, DOWN), DOWN)] = out.reshape(side, side, pad, DOWN)

        for c in third(e):
            c.start()

    pa[...] = jnp.zeros_like(pa)
    pb[...] = jnp.zeros_like(pb)

    @pl.loop(0, local)
    def _(e):
        for c in third(e):
            c.wait()
        for p, g, back in ((pa, ga, ca), (pb, gb, cb)):
            for s in range(side):
                weigh = jnp.where(token == g[s, pl.ds(e, 1), :], g[s, pl.ds(local + e, 1), :], 0.0).astype(BF16)
                p[s] += dot(weigh, back[e, s].reshape(side * pad, half))

    last = []
    for axis, (p, t, q) in enumerate(((pa, ta, qa), (pb, tb, qb))):
        t[...] = p[...].astype(BF16)
        mine = (at.x, at.y)[axis]
        for d in range(1, side):
            c, device = at.peer(axis, d)
            last.append(remote(t.at[c], q.at[mine], (s4s, s4r), axis * side + d, device))
    for c in last:
        c.start()
    for c in last:
        c.wait()
    for axis, (p, q, lo) in enumerate(((pa, qa, 0), (pb, qb, half))):
        mine = (at.x, at.y)[axis]
        y = p[mine]
        for d in range(1, side):
            y += q[at.peer(axis, d)[0]].astype(F32)
        y_ref[:, lo : lo + half] = (y + sh[:, lo : lo + half]).astype(BF16)


def solution(mesh):
    side = math.isqrt(mesh.shape["ep"])
    vmem, hbm = pl.BlockSpec(memory_space=pltpu.VMEM), pl.BlockSpec(memory_space=pl.ANY)
    dma = lambda *n: pltpu.SemaphoreType.DMA(n)

    def body(x, expert, slot, gate, w_gate, w_up, w_down, s_gate, s_up, s_down):
        x, expert, slot, gate = x[0, 0], expert[0, 0], slot[0, 0], gate[0, 0]
        tokens, top = expert.shape
        d_model = x.shape[1]
        local, _, ff = w_gate.shape
        slots = 5 * tokens * top // (4 * local * side * side)
        pad = -(-slots // 16) * 16
        half = d_model // 2
        assert tokens <= 256
        staged = pltpu.VMEM((local, side, side, pad, half), BF16)
        gathered = pltpu.VMEM((side, tokens, half), BF16)
        added = pltpu.VMEM((side, tokens, half), F32)
        table = pltpu.VMEM((side, 2 * local, side * pad), F32)
        y = pl.pallas_call(
            functools.partial(layer_kernel, side, slots),
            out_shape=jax.ShapeDtypeStruct((tokens, d_model), BF16),
            in_specs=[vmem] * 4 + [hbm] * 6,
            out_specs=vmem,
            scratch_shapes=[table] * 4
            + [gathered] * 2
            + [staged] * 2
            + [pltpu.VMEM((local, side, side, pad, d_model), BF16), pltpu.VMEM((side * side * pad, ff), BF16)]
            + [staged] * 2
            + [added] * 2
            + [gathered] * 4
            + [
                pltpu.VMEM((tokens, d_model), F32),
                pltpu.VMEM((DEPTH, d_model, 2 * UP), BF16),
                pltpu.VMEM((2, ff, DOWN), BF16),
            ]
            + [dma(4 * side)] * 2
            + [dma(2 * local * side)] * 4
            + [dma(2 * side)] * 2
            + [dma(local, 2)] * 2
            + [dma(DEPTH, 2), dma(2)],
            compiler_params=pltpu.CompilerParams(collective_id=0, has_side_effects=True, vmem_limit_bytes=67043328),
        )(x, expert.T, slot.T, gate.T, s_gate, s_up, s_down, w_gate, w_up, w_down)
        return y[None, None]

    token = P("dp", "ep")
    return jax.shard_map(
        body,
        mesh=mesh,
        in_specs=(token,) * 4 + (P("ep"),) * 3 + (P(),) * 3,
        out_specs=token,
        check_vma=False,
    )
```

```python
import functools
import math

import jax
import jax.numpy as jnp
from jax import lax
from jax.experimental import pallas as pl
from jax.experimental.pallas import tpu as pltpu
from jax.sharding import PartitionSpec as P

MESH = pl.DeviceIdType.MESH
F32, BF16 = jnp.float32, jnp.bfloat16
UP, DOWN = 128, 1024
DEPTH = 3


def dot(a, b, contract=((1,), (0,))):
    return lax.dot_general(a, b, (contract, ((), ())), preferred_element_type=F32)


def gated(g, u):
    return (jax.nn.silu(g) * u).astype(BF16)


class Place:
    def __init__(self, side):
        me = lax.axis_index("ep")
        self.side = side
        self.x, self.y = lax.div(me, side), lax.rem(me, side)

    def peer(self, axis, d):
        if axis == 0:
            c = lax.rem(self.x + d, self.side)
            return c, {"ep": c * self.side + self.y}
        c = lax.rem(self.y + d, self.side)
        return c, {"ep": self.x * self.side + c}

    def greet(self):
        barrier = pltpu.get_barrier_semaphore()
        for axis in (0, 1):
            for d in range(1, self.side):
                pl.semaphore_signal(barrier, inc=1, device_id=self.peer(axis, d)[1], device_id_type=MESH)
        pl.semaphore_wait(barrier, 2 * (self.side - 1))


def remote(src, dst, sems, k, device):
    return pltpu.make_async_remote_copy(
        src_ref=src, dst_ref=dst, send_sem=sems[0].at[k], recv_sem=sems[1].at[k], device_id=device, device_id_type=MESH
    )


def tables(side, local, pad, slots, expert, slot, gate, ra, rb):
    top, _, tokens = expert.shape
    token = lax.broadcasted_iota(jnp.int32, (1, tokens), 1).astype(F32) + 1.0
    lines = lax.broadcasted_iota(jnp.int32, (side * local, tokens), 0)
    places = lax.broadcasted_iota(jnp.int32, (side * pad, tokens), 0)
    sums = [0.0, 0.0]
    for k in range(top):
        ex, sl = expert[k], slot[k]
        weight = gate[k].astype(BF16).astype(F32)
        e, device = lax.rem(ex, local), lax.div(ex, local)
        where = lax.div(device, side), lax.rem(device, side)
        for axis in (0, 1):
            line = (lines == where[axis] * local + e).astype(F32).astype(BF16)
            hit = places == jnp.where(sl < slots, where[1 - axis] * pad + sl, -1)
            held = jnp.concatenate([jnp.where(hit, token, 0.0), jnp.where(hit, weight, 0.0)]).astype(BF16)
            sums[axis] += dot(line, held, ((1,), (1,)))
    for held, r in zip(sums, (ra, rb)):
        for c in range(side):
            r[c, :local] = held[c * local : (c + 1) * local, : side * pad]
            r[c, local:] = held[c * local : (c + 1) * local, side * pad :]


def layer_kernel(side, slots, x_ref, ex_ref, sl_ref, gt_ref, sg_ref, su_ref, sd_ref, wg_ref, wu_ref, wd_ref, y_ref,
                 ra, rb, ga, gb, gxa, gxb, sta, stb, z, h, ca, cb, pa, pb, ta, tb, qa, qb, va, vb, sh, wup, wdn,
                 s0s, s0r, s1s, s1r, s2s, s2r, s3s, s3r, s4s, s4r, loc2, loc3, sup, sdn):
    at = Place(side)
    tokens, half = gxa.shape[1:]
    local, pad = z.shape[0], z.shape[3]
    rows = side * side * pad
    d_model, ff = wg_ref.shape[1:]
    ups, downs = ff // UP, d_model // DOWN

    def up_tile(n):
        e, i = lax.div(n, ups), lax.rem(n, ups)
        k = lax.rem(n, DEPTH)
        cols = pl.ds(pl.multiple_of(i * UP, UP), UP)
        return [
            pltpu.make_async_copy(w.at[e, :, cols], wup.at[k, :, pl.ds(j * UP, UP)], sup.at[k, j])
            for j, w in enumerate((wg_ref, wu_ref))
        ]

    def down_tile(n):
        e, i = lax.div(n, downs), lax.rem(n, downs)
        k = lax.rem(n, 2)
        cols = pl.ds(pl.multiple_of(i * DOWN, DOWN), DOWN)
        return pltpu.make_async_copy(wd_ref.at[e, :, cols], wdn.at[k], sdn.at[k])

    at.greet()

    right, left = 1, side - 1
    cut = tokens // 2
    low, high = pl.ds(0, cut), pl.ds(cut, cut)
    sides = ((0, gxa, ra, ga, at.x), (half, gxb, rb, gb, at.y))
    first, onward, small = [], [], []
    for axis, (lo, gx, r, g, mine) in enumerate(sides):
        cols = pl.ds(lo, half)
        for i, (d, piece) in enumerate(((right, low), (left, high), (right, high), (left, low))):
            device = at.peer(axis, d)[1]
            first.append(remote(x_ref.at[piece, cols], gx.at[mine, piece], (s1s, s1r), axis * 6 + i, device))
        for i, (d, piece) in enumerate(((right, low), (left, high))):
            origin = at.peer(axis, side - d)[0]
            rows_on = gx.at[origin, piece]
            onward.append(remote(rows_on, rows_on, (s1s, s1r), axis * 6 + 4 + i, at.peer(axis, d)[1]))
        for d in range(1, side):
            c, device = at.peer(axis, d)
            small.append(remote(r.at[c], g.at[mine], (s0s, s0r), axis * side + d, device))
    for i in (0, 1, 4, 5, 2, 3, 6, 7):
        first[i].start()
    tables(side, local, pad, slots, ex_ref, sl_ref, gt_ref, ra, rb)
    for c in small:
        c.start()
    ga[at.x] = ra[at.x]
    gb[at.y] = rb[at.y]

    token = lax.broadcasted_iota(jnp.int32, (tokens, side * pad), 0).astype(F32) + 1.0

    def pick(e, axis, c, x):
        g, st = ((ga, sta), (gb, stb))[axis]
        hit = (token == g[c, pl.ds(e, 1), :]).astype(F32).astype(BF16)
        picked = dot(hit, x, ((0,), (0,))).astype(BF16)
        for to in range(side):
            st[e, to, c] = picked[to * pad : (to + 1) * pad]

    def second(e, origin=None):
        out = []
        for axis, st in enumerate((sta, stb)):
            piece = slice(None) if origin is None else at.peer(axis, origin)[0]
            for d in range(side):
                c, device = at.peer(1 - axis, d)
                src = st.at[e, c, piece]
                if axis == 0:
                    dst = z.at[e, at.y, piece, :, pl.ds(0, half)]
                else:
                    dst = z.at[e, piece, at.x, :, pl.ds(half, half)]
                if d == 0:
                    out.append(pltpu.make_async_copy(src, dst, loc2.at[e, axis]))
                else:
                    out.append(remote(src, dst, (s2s, s2r), (e * 2 + axis) * side + d, device))
        return out

    @pl.loop(0, local)
    def _(e):
        pick(e, 0, at.x, x_ref[:, :half])
        pick(e, 1, at.y, x_ref[:, half:])

    for i in (0, 1, 4, 5):
        first[i].wait_recv()
    for c in onward:
        c.start()

    @pl.loop(0, local)
    def _(e):
        for c in second(e, 0):
            c.start()

    sh[...] = jnp.zeros_like(sh)

    def shared(g_ref, u_ref, d_ref):
        x = x_ref[...]
        sh[...] += dot(gated(dot(x, g_ref[...]), dot(x, u_ref[...])), d_ref[...])

    tile = 256 if sg_ref.shape[1] % 256 == 0 else 128
    pltpu.emit_pipeline(
        shared,
        grid=(sg_ref.shape[1] // tile,),
        in_specs=[
            pl.BlockSpec((d_model, tile), lambda i: (0, i)),
            pl.BlockSpec((d_model, tile), lambda i: (0, i)),
            pl.BlockSpec((tile, d_model), lambda i: (i, 0)),
        ],
    )(sg_ref, su_ref, sd_ref)

    for n in range(DEPTH - 1):
        for c in up_tile(jnp.int32(n)):
            c.start()
    down_tile(jnp.int32(0)).start()
    for i in (2, 3, 6, 7):
        first[i].wait_recv()
    for c in onward + small:
        c.wait_recv()

    @pl.loop(0, local)
    def _(e):
        for d in range(1, side):
            for axis, gx in enumerate((gxa, gxb)):
                c = at.peer(axis, d)[0]
                pick(e, axis, c, gx[c])
            for c in second(e, d):
                c.start()

    for c in first + onward + small:
        c.wait_send()

    final = local - 1

    def third(e, origin=None):
        out = []
        for axis in (0, 1):
            piece = slice(None) if origin is None else at.peer(axis, origin)[0]
            for d in range(side):
                c, device = at.peer(1 - axis, d)
                if axis == 0:
                    src, dst = z.at[e, c, piece, :, pl.ds(0, half)], ca.at[e, piece, at.y]
                else:
                    src, dst = z.at[e, piece, c, :, pl.ds(half, half)], cb.at[e, piece, at.x]
                k = (e * 2 + axis) * side + d if origin is None else ((local + origin) * 2 + axis) * side + d
                if d == 0:
                    own = loc3.at[e if origin is None else local + origin, axis]
                    out.append(pltpu.make_async_copy(src, dst, own))
                else:
                    out.append(remote(src, dst, (s3s, s3r), k, device))
        return out

    def expert(e):
        for c in second(e):
            c.wait()

        @pl.loop(0, ups)
        def _(i):
            n = e * ups + i

            @pl.when(n + DEPTH - 1 < local * ups)
            def _():
                for c in up_tile(n + DEPTH - 1):
                    c.start()

            for c in up_tile(n):
                c.wait()
            gu = dot(z[e].reshape(rows, d_model), wup[lax.rem(n, DEPTH)])
            h[:, pl.ds(pl.multiple_of(i * UP, UP), UP)] = gated(gu[:, :UP], gu[:, UP:])

        @pl.loop(0, downs)
        def _(i):
            n = e * downs + i

            @pl.when(n + 1 < local * downs)
            def _():
                down_tile(n + 1).start()

            down_tile(n).wait()
            out = dot(h[...], wdn[lax.rem(n, 2)]).astype(BF16)
            z[e, :, :, :, pl.ds(pl.multiple_of(i * DOWN, DOWN), DOWN)] = out.reshape(side, side, pad, DOWN)

        @pl.when(e < final)
        def _():
            for c in third(e):
                c.start()

    pl.loop(0, local)(expert)
    order = (side // 2, right, left, 0)
    for d in order:
        for c in third(final, d):
            c.start()

    def add(e, axis, c):
        g, back, p = ((ga, ca, pa), (gb, cb, pb))[axis]
        weigh = jnp.where(token == g[c, pl.ds(e, 1), :], g[c, pl.ds(local + e, 1), :], 0.0).astype(BF16)
        p[c] += dot(weigh, back[e, c].reshape(side * pad, half))

    pa[...] = jnp.zeros_like(pa)
    pb[...] = jnp.zeros_like(pb)

    @pl.loop(0, final)
    def _(e):
        for c in third(e):
            c.wait()
        for s in range(side):
            add(e, 0, s)
            add(e, 1, s)

    waits = []

    def send(axis, i, src, dst, d):
        c = remote(src, dst, (s4s, s4r), axis * 6 + i, at.peer(axis, d)[1])
        c.start()
        waits.append(c)
        return c

    through = {}
    for d in order:
        for c in third(final, d):
            c.wait()
        for axis, (p, t, q, v) in enumerate(((pa, ta, qa, va), (pb, tb, qb, vb))):
            c = at.peer(axis, d)[0]
            add(final, axis, c)
            if d == side // 2:
                t[0] = p[c].astype(BF16)
                through[axis, right] = send(axis, 0, t.at[0, low], v.at[0], right)
                through[axis, left] = send(axis, 1, t.at[0, high], v.at[1], left)
            elif d == right:
                t[1, high] = p[c, high].astype(BF16)
                send(axis, 2, t.at[1, high], q.at[0, high], right)
            elif d == left:
                t[2, low] = p[c, low].astype(BF16)
                send(axis, 3, t.at[2, low], q.at[1, low], left)
    for axis, (p, t, q, v) in enumerate(((pa, ta, qa, va), (pb, tb, qb, vb))):
        through[axis, right].wait_recv()
        t[1, low] = (p[at.peer(axis, right)[0], low] + v[0].astype(F32)).astype(BF16)
        send(axis, 4, t.at[1, low], q.at[0, low], right)
        through[axis, left].wait_recv()
        t[2, high] = (p[at.peer(axis, left)[0], high] + v[1].astype(F32)).astype(BF16)
        send(axis, 5, t.at[2, high], q.at[1, high], left)
    for axis, (p, lo) in enumerate(((pa, 0), (pb, half))):
        cols = slice(lo, lo + half)
        sh[:, cols] = sh[:, cols] + p[(at.x, at.y)[axis]]
    for c in waits:
        c.wait_send()
        if all(c is not t for t in through.values()):
            c.wait_recv()
    for q, lo in ((qa, 0), (qb, half)):
        y_ref[:, lo : lo + half] = (sh[:, lo : lo + half] + q[0].astype(F32) + q[1].astype(F32)).astype(BF16)


def solution(mesh):
    side = math.isqrt(mesh.shape["ep"])
    vmem, hbm = pl.BlockSpec(memory_space=pltpu.VMEM), pl.BlockSpec(memory_space=pl.ANY)
    dma = lambda *n: pltpu.SemaphoreType.DMA(n)

    def body(x, expert, slot, gate, w_gate, w_up, w_down, s_gate, s_up, s_down):
        x, expert, slot, gate = x[0, 0], expert[0, 0], slot[0, 0], gate[0, 0]
        tokens, top = expert.shape
        d_model = x.shape[1]
        local, _, ff = w_gate.shape
        slots = 5 * tokens * top // (4 * local * side * side)
        pad = -(-slots // 16) * 16
        half = d_model // 2
        assert tokens <= 256
        staged = pltpu.VMEM((local, side, side, pad, half), BF16)
        gathered = pltpu.VMEM((side, tokens, half), BF16)
        added = pltpu.VMEM((side, tokens, half), F32)
        table = pltpu.VMEM((side, 2 * local, side * pad), F32)
        y = pl.pallas_call(
            functools.partial(layer_kernel, side, slots),
            out_shape=jax.ShapeDtypeStruct((tokens, d_model), BF16),
            in_specs=[vmem] * 4 + [hbm] * 6,
            out_specs=vmem,
            scratch_shapes=[table] * 4
            + [gathered] * 2
            + [staged] * 2
            + [pltpu.VMEM((local, side, side, pad, d_model), BF16), pltpu.VMEM((side * side * pad, ff), BF16)]
            + [staged] * 2
            + [added] * 2
            + [pltpu.VMEM((3, tokens, half), BF16)] * 2
            + [pltpu.VMEM((2, tokens, half), BF16)] * 2
            + [pltpu.VMEM((2, tokens // 2, half), BF16)] * 2
            + [
                pltpu.VMEM((tokens, d_model), F32),
                pltpu.VMEM((DEPTH, d_model, 2 * UP), BF16),
                pltpu.VMEM((2, ff, DOWN), BF16),
            ]
            + [dma(2 * side)] * 2
            + [dma(12)] * 2
            + [dma(2 * local * side)] * 2
            + [dma(2 * (local + side) * side)] * 2
            + [dma(12)] * 2
            + [dma(local, 2), dma(local + side, 2)]
            + [dma(DEPTH, 2), dma(2)],
            compiler_params=pltpu.CompilerParams(collective_id=0, has_side_effects=True, vmem_limit_bytes=67043328),
        )(x, expert.T[:, None], slot.T[:, None], gate.T[:, None], s_gate, s_up, s_down, w_gate, w_up, w_down)
        return y[None, None]

    token = P("dp", "ep")
    return jax.shard_map(
        body,
        mesh=mesh,
        in_specs=(token,) * 4 + (P("ep"),) * 3 + (P(),) * 3,
        out_specs=token,
        check_vma=False,
    )
```

```python
import functools
import math

import jax
import jax.numpy as jnp
from jax import lax
from jax.experimental import pallas as pl
from jax.experimental.pallas import tpu as pltpu
from jax.sharding import PartitionSpec as P

MESH = pl.DeviceIdType.MESH
F32, BF16 = jnp.float32, jnp.bfloat16
UP, DOWN = 128, 1024
DEPTH = 3


def dot(a, b, contract=((1,), (0,))):
    return lax.dot_general(a, b, (contract, ((), ())), preferred_element_type=F32)


def gated(g, u):
    return (jax.nn.silu(g) * u).astype(BF16)


class Place:
    def __init__(self, side):
        me = lax.axis_index("ep")
        self.side = side
        self.x, self.y = lax.div(me, side), lax.rem(me, side)

    def peer(self, axis, d):
        if axis == 0:
            c = lax.rem(self.x + d, self.side)
            return c, {"ep": c * self.side + self.y}
        c = lax.rem(self.y + d, self.side)
        return c, {"ep": self.x * self.side + c}

    def greet(self):
        barrier = pltpu.get_barrier_semaphore()
        for axis in (0, 1):
            for d in range(1, self.side):
                pl.semaphore_signal(barrier, inc=1, device_id=self.peer(axis, d)[1], device_id_type=MESH)
        pl.semaphore_wait(barrier, 2 * (self.side - 1))


def remote(src, dst, sems, k, device):
    return pltpu.make_async_remote_copy(
        src_ref=src, dst_ref=dst, send_sem=sems[0].at[k], recv_sem=sems[1].at[k], device_id=device, device_id_type=MESH
    )


def tables(side, local, pad, slots, expert, slot, gate, ra, rb):
    top, _, tokens = expert.shape
    token = lax.broadcasted_iota(jnp.int32, (1, tokens), 1).astype(F32) + 1.0
    lines = lax.broadcasted_iota(jnp.int32, (side * local, tokens), 0)
    places = lax.broadcasted_iota(jnp.int32, (side * pad, tokens), 0)
    sums = [0.0, 0.0]
    for k in range(top):
        ex, sl = expert[k], slot[k]
        weight = gate[k].astype(BF16).astype(F32)
        e, device = lax.rem(ex, local), lax.div(ex, local)
        where = lax.div(device, side), lax.rem(device, side)
        for axis in (0, 1):
            line = (lines == where[axis] * local + e).astype(F32).astype(BF16)
            hit = places == jnp.where(sl < slots, where[1 - axis] * pad + sl, -1)
            held = jnp.concatenate([jnp.where(hit, token, 0.0), jnp.where(hit, weight, 0.0)]).astype(BF16)
            sums[axis] += dot(line, held, ((1,), (1,)))
    for held, r in zip(sums, (ra, rb)):
        for c in range(side):
            r[c, :local] = held[c * local : (c + 1) * local, : side * pad]
            r[c, local:] = held[c * local : (c + 1) * local, side * pad :]


def layer_kernel(side, slots, x_ref, ex_ref, sl_ref, gt_ref, sg_ref, su_ref, sd_ref, wg_ref, wu_ref, wd_ref, y_ref,
                 ra, rb, ga, gb, gxa, gxb, sta, stb, z, h, ca, cb, pa, pb, ta, tb, qa, qb, va, vb, sh, wup, wdn,
                 s0s, s0r, s1s, s1r, s2s, s2r, s3s, s3r, s4s, s4r, loc2, loc3, sup, sdn):
    at = Place(side)
    tokens, half = gxa.shape[1:]
    local, pad = z.shape[0], z.shape[3]
    rows = side * side * pad
    d_model, ff = wg_ref.shape[1:]
    ups, downs = ff // UP, d_model // DOWN

    def up_tile(n):
        e, i = lax.div(n, ups), lax.rem(n, ups)
        k = lax.rem(n, DEPTH)
        cols = pl.ds(pl.multiple_of(i * UP, UP), UP)
        return [
            pltpu.make_async_copy(w.at[e, :, cols], wup.at[k, :, pl.ds(j * UP, UP)], sup.at[k, j])
            for j, w in enumerate((wg_ref, wu_ref))
        ]

    def down_tile(n):
        e, i = lax.div(n, downs), lax.rem(n, downs)
        k = lax.rem(n, 2)
        cols = pl.ds(pl.multiple_of(i * DOWN, DOWN), DOWN)
        return pltpu.make_async_copy(wd_ref.at[e, :, cols], wdn.at[k], sdn.at[k])

    at.greet()

    right, left = 1, side - 1
    cut = tokens // 2
    low, high = pl.ds(0, cut), pl.ds(cut, cut)
    sides = ((0, gxa, ra, ga, at.x), (half, gxb, rb, gb, at.y))
    first, onward, small = [], [], []
    for axis, (lo, gx, r, g, mine) in enumerate(sides):
        cols = pl.ds(lo, half)
        for i, (d, piece) in enumerate(((right, low), (left, high), (right, high), (left, low))):
            device = at.peer(axis, d)[1]
            first.append(remote(x_ref.at[piece, cols], gx.at[mine, piece], (s1s, s1r), axis * 6 + i, device))
        for i, (d, piece) in enumerate(((right, low), (left, high))):
            origin = at.peer(axis, side - d)[0]
            rows_on = gx.at[origin, piece]
            onward.append(remote(rows_on, rows_on, (s1s, s1r), axis * 6 + 4 + i, at.peer(axis, d)[1]))
        for d in range(1, side):
            c, device = at.peer(axis, d)
            small.append(remote(r.at[c], g.at[mine], (s0s, s0r), axis * side + d, device))
    for i in (0, 1, 4, 5, 2, 3, 6, 7):
        first[i].start()
    tables(side, local, pad, slots, ex_ref, sl_ref, gt_ref, ra, rb)
    for c in small:
        c.start()
    ga[at.x] = ra[at.x]
    gb[at.y] = rb[at.y]

    token = lax.broadcasted_iota(jnp.int32, (tokens, side * pad), 0).astype(F32) + 1.0

    def pick(e, axis, c, x):
        g, st = ((ga, sta), (gb, stb))[axis]
        hit = (token == g[c, pl.ds(e, 1), :]).astype(F32).astype(BF16)
        picked = dot(hit, x, ((0,), (0,))).astype(BF16)
        for to in range(side):
            st[e, to, c] = picked[to * pad : (to + 1) * pad]

    def second(e, origin=None):
        out = []
        for axis, st in enumerate((sta, stb)):
            piece = slice(None) if origin is None else at.peer(axis, origin)[0]
            for d in range(side):
                c, device = at.peer(1 - axis, d)
                src = st.at[e, c, piece]
                if axis == 0:
                    dst = z.at[e, at.y, piece, :, pl.ds(0, half)]
                else:
                    dst = z.at[e, piece, at.x, :, pl.ds(half, half)]
                if d == 0:
                    out.append(pltpu.make_async_copy(src, dst, loc2.at[e, axis]))
                else:
                    out.append(remote(src, dst, (s2s, s2r), (e * 2 + axis) * side + d, device))
        return out

    @pl.loop(0, local)
    def _(e):
        pick(e, 0, at.x, x_ref[:, :half])
        pick(e, 1, at.y, x_ref[:, half:])

    for i in (0, 1, 4, 5):
        first[i].wait_recv()
    for c in onward:
        c.start()

    @pl.loop(0, local)
    def _(e):
        for c in second(e, 0):
            c.start()

    sh[...] = jnp.zeros_like(sh)

    def shared(g_ref, u_ref, d_ref):
        x = x_ref[...]
        sh[...] += dot(gated(dot(x, g_ref[...]), dot(x, u_ref[...])), d_ref[...])

    tile = 256 if sg_ref.shape[1] % 256 == 0 else 128
    pltpu.emit_pipeline(
        shared,
        grid=(sg_ref.shape[1] // tile,),
        in_specs=[
            pl.BlockSpec((d_model, tile), lambda i: (0, i)),
            pl.BlockSpec((d_model, tile), lambda i: (0, i)),
            pl.BlockSpec((tile, d_model), lambda i: (i, 0)),
        ],
    )(sg_ref, su_ref, sd_ref)

    for n in range(DEPTH - 1):
        for c in up_tile(jnp.int32(n)):
            c.start()
    down_tile(jnp.int32(0)).start()
    for i in (2, 3, 6, 7):
        first[i].wait_recv()
    for c in onward + small:
        c.wait_recv()

    @pl.loop(0, local)
    def _(e):
        for d in range(1, side):
            for axis, gx in enumerate((gxa, gxb)):
                c = at.peer(axis, d)[0]
                pick(e, axis, c, gx[c])
            for c in second(e, d):
                c.start()

    for c in first + onward + small:
        c.wait_send()

    final = local - 1

    def third(e, origin=None):
        out = []
        for axis in (0, 1):
            piece = slice(None) if origin is None else at.peer(axis, origin)[0]
            for d in range(side):
                c, device = at.peer(1 - axis, d)
                if axis == 0:
                    src, dst = z.at[e, c, piece, :, pl.ds(0, half)], ca.at[e, piece, at.y]
                else:
                    src, dst = z.at[e, piece, c, :, pl.ds(half, half)], cb.at[e, piece, at.x]
                k = (e * 2 + axis) * side + d if origin is None else ((local + origin) * 2 + axis) * side + d
                if d == 0:
                    own = loc3.at[e if origin is None else local + origin, axis]
                    out.append(pltpu.make_async_copy(src, dst, own))
                else:
                    out.append(remote(src, dst, (s3s, s3r), k, device))
        return out

    def expert(e):
        for c in second(e):
            c.wait()

        @pl.loop(0, ups)
        def _(i):
            n = e * ups + i

            @pl.when(n + DEPTH - 1 < local * ups)
            def _():
                for c in up_tile(n + DEPTH - 1):
                    c.start()

            for c in up_tile(n):
                c.wait()
            gu = dot(z[e].reshape(rows, d_model), wup[lax.rem(n, DEPTH)])
            h[:, pl.ds(pl.multiple_of(i * UP, UP), UP)] = gated(gu[:, :UP], gu[:, UP:])

        @pl.loop(0, downs)
        def _(i):
            n = e * downs + i

            @pl.when(n + 1 < local * downs)
            def _():
                down_tile(n + 1).start()

            down_tile(n).wait()
            out = dot(h[...], wdn[lax.rem(n, 2)]).astype(BF16)
            z[e, :, :, :, pl.ds(pl.multiple_of(i * DOWN, DOWN), DOWN)] = out.reshape(side, side, pad, DOWN)

        @pl.when(e < final)
        def _():
            for c in third(e):
                c.start()

    pl.loop(0, local)(expert)
    order = (side // 2, right, left, 0)
    for d in order:
        for c in third(final, d):
            c.start()

    def add(e, axis, c):
        g, back, p = ((ga, ca, pa), (gb, cb, pb))[axis]
        weigh = jnp.where(token == g[c, pl.ds(e, 1), :], g[c, pl.ds(local + e, 1), :], 0.0).astype(BF16)
        p[c] += dot(weigh, back[e, c].reshape(side * pad, half))

    pa[...] = jnp.zeros_like(pa)
    pb[...] = jnp.zeros_like(pb)

    @pl.loop(0, final)
    def _(e):
        for c in third(e):
            c.wait()
        for s in range(side):
            add(e, 0, s)
            add(e, 1, s)

    waits = []

    def send(axis, i, src, dst, d):
        c = remote(src, dst, (s4s, s4r), axis * 6 + i, at.peer(axis, d)[1])
        c.start()
        waits.append(c)
        return c

    through = {}
    for d in order:
        for c in third(final, d):
            c.wait()
        for axis, (p, t, q, v) in enumerate(((pa, ta, qa, va), (pb, tb, qb, vb))):
            c = at.peer(axis, d)[0]
            add(final, axis, c)
            if d == side // 2:
                t[0] = p[c].astype(BF16)
                through[axis, right] = send(axis, 0, t.at[0, low], v.at[0], right)
                through[axis, left] = send(axis, 1, t.at[0, high], v.at[1], left)
            elif d == right:
                t[1, high] = p[c, high].astype(BF16)
                send(axis, 2, t.at[1, high], q.at[0, high], right)
            elif d == left:
                t[2, low] = p[c, low].astype(BF16)
                send(axis, 3, t.at[2, low], q.at[1, low], left)
    for axis, (p, t, q, v) in enumerate(((pa, ta, qa, va), (pb, tb, qb, vb))):
        through[axis, right].wait_recv()
        t[1, low] = (p[at.peer(axis, right)[0], low] + v[0].astype(F32)).astype(BF16)
        send(axis, 4, t.at[1, low], q.at[0, low], right)
        through[axis, left].wait_recv()
        t[2, high] = (p[at.peer(axis, left)[0], high] + v[1].astype(F32)).astype(BF16)
        send(axis, 5, t.at[2, high], q.at[1, high], left)
    for axis, (p, lo) in enumerate(((pa, 0), (pb, half))):
        cols = slice(lo, lo + half)
        sh[:, cols] = sh[:, cols] + p[(at.x, at.y)[axis]]
    for c in waits:
        c.wait_send()
        if all(c is not t for t in through.values()):
            c.wait_recv()
    for q, lo in ((qa, 0), (qb, half)):
        y_ref[:, lo : lo + half] = (sh[:, lo : lo + half] + q[0].astype(F32) + q[1].astype(F32)).astype(BF16)


def solution(mesh):
    side = math.isqrt(mesh.shape["ep"])
    vmem, hbm = pl.BlockSpec(memory_space=pltpu.VMEM), pl.BlockSpec(memory_space=pl.ANY)
    dma = lambda *n: pltpu.SemaphoreType.DMA(n)

    def body(x, expert, slot, gate, w_gate, w_up, w_down, s_gate, s_up, s_down):
        x, tokens, top = x[0, 0], *expert.shape[2:]
        by_choice = lambda v: v[0].transpose(2, 0, 1)
        d_model = x.shape[1]
        local, _, ff = w_gate.shape
        slots = 5 * tokens * top // (4 * local * side * side)
        pad = -(-slots // 16) * 16
        half = d_model // 2
        assert tokens <= 256
        staged = pltpu.VMEM((local, side, side, pad, half), BF16)
        gathered = pltpu.VMEM((side, tokens, half), BF16)
        added = pltpu.VMEM((side, tokens, half), F32)
        table = pltpu.VMEM((side, 2 * local, side * pad), F32)
        y = pl.pallas_call(
            functools.partial(layer_kernel, side, slots),
            out_shape=jax.ShapeDtypeStruct((tokens, d_model), BF16),
            in_specs=[vmem] * 4 + [hbm] * 6,
            out_specs=vmem,
            scratch_shapes=[table] * 4
            + [gathered] * 2
            + [staged] * 2
            + [pltpu.VMEM((local, side, side, pad, d_model), BF16), pltpu.VMEM((side * side * pad, ff), BF16)]
            + [staged] * 2
            + [added] * 2
            + [pltpu.VMEM((3, tokens, half), BF16)] * 2
            + [pltpu.VMEM((2, tokens, half), BF16)] * 2
            + [pltpu.VMEM((2, tokens // 2, half), BF16)] * 2
            + [
                pltpu.VMEM((tokens, d_model), F32),
                pltpu.VMEM((DEPTH, d_model, 2 * UP), BF16),
                pltpu.VMEM((2, ff, DOWN), BF16),
            ]
            + [dma(2 * side)] * 2
            + [dma(12)] * 2
            + [dma(2 * local * side)] * 2
            + [dma(2 * (local + side) * side)] * 2
            + [dma(12)] * 2
            + [dma(local, 2), dma(local + side, 2)]
            + [dma(DEPTH, 2), dma(2)],
            compiler_params=pltpu.CompilerParams(collective_id=0, has_side_effects=True, vmem_limit_bytes=67043328),
        )(x, by_choice(expert), by_choice(slot), by_choice(gate), s_gate, s_up, s_down, w_gate, w_up, w_down)
        return y[None, None]

    token = P("dp", "ep")
    return jax.shard_map(
        body,
        mesh=mesh,
        in_specs=(token,) * 4 + (P("ep"),) * 3 + (P(),) * 3,
        out_specs=token,
        check_vma=False,
    )
```
